32 devices in a mesh: seq: 16 (over z, x, core), head: 2 (over y).
Axes of the slice: x: 2, y: 2, z: 4, core: 2. Of those that a mesh axis runs over, the one named last changes fastest.
Arguments:
- prompt_token_query: bfloat16 [512, 8192], P('seq', 'head'), may hold values from -6 to 6
- prompt_token_key: bfloat16 [512, 1024], P('seq', 'head'), may hold values from -6 to 6
- prompt_token_value: bfloat16 [512, 1024], P('seq', 'head'), may hold values from -6 to 6
- response_query_slots: bfloat16 [3072, 8192], P('seq', 'head'), may hold values from -160 to 160
- response_key_slots: bfloat16 [3072, 1024], P('seq', 'head'), may hold values from -6 to 6
- response_value_slots: bfloat16 [3072, 1024], P('seq', 'head'), may hold values from -6 to 6
- lengths: int32 [4], replicated, may hold values from 1 to 8, 16 in all
- block_table: int32 [16], replicated, may hold values from 0 to 15, each once
Outputs:
- prompt_out: bfloat16 [512, 8192], P(('seq', 'head'))
- answer_out: bfloat16 [3072, 8192], P(('seq', 'head'))
The draws below stay inside these ranges and needn't reach their ends.
Inputs may be any that keep to these rules, and one draw needn't show every extreme that they name: `lengths`: they sum to 16; the largest is exactly 8. `block_table`: A permutation of 0 to 15.
All inputs are finite; a program needn't handle non-finite values.
Results may differ from the reference program's by a relative error of at most 0.007.
Values may be sent and summed in bfloat16 or wider, within the bound.
A program may use at most 64 MiB of HBM per device.

```python
import math
import jax
import jax.numpy as jnp
import numpy as np
from jax import lax

QUERY_HEADS = 64
KEY_VALUE_HEADS = 8
HEAD_SIZE = 128
RESPONSE_BLOCK = 192
PROMPT_PER_SEQ = 32
MEMBERS = 4
RESPONSE_COUNT = 16
LONGEST_BLOCKS = 8
PROMPT_TOKENS = 512
RESPONSE_TOKENS = 3072
N_SEQ = 16


def paired_keys(key):
    regular_portion = jnp.clip(jax.random.normal(jax.random.fold_in(key, 7001), (PROMPT_TOKENS, KEY_VALUE_HEADS, HEAD_SIZE), jnp.float32), -6.0, 6.0)
    return regular_portion


def draw_prompt_token_key(key, part):
    key_lookup_table = paired_keys(key)
    return key_lookup_table.reshape(PROMPT_TOKENS, KEY_VALUE_HEADS * HEAD_SIZE).astype(jnp.bfloat16)


def draw_response_query_slots(key, part):
    regular_portion = jnp.clip(jax.random.normal(jax.random.fold_in(key, 7003), (RESPONSE_TOKENS, QUERY_HEADS, HEAD_SIZE), jnp.float32), -6.0, 6.0)
    return regular_portion.reshape(RESPONSE_TOKENS, QUERY_HEADS * HEAD_SIZE).astype(jnp.bfloat16)


def shard_levels(key, shape, shards, smallest, high):
    def one(dim, parts):
        steps = jax.random.uniform(jax.random.fold_in(jax.random.fold_in(key, 6), dim), (parts,), jnp.float32, smallest / len(shards), high / len(shards))
        return jnp.repeat(jnp.exp(steps), shape[dim] // parts).reshape((-1,) + (1,) * (len(shape) - dim - 1))

    loudness = one(*shards[0])
    for cut in shards[1:]:
        loudness = loudness * one(*cut)
    return loudness


def length_profile(count, total, most, skew):
    portions = [(1 << 20) // math.isqrt(grade ** skew) + 1 for grade in range(2, count + 1)]
    surplus, given = total - most - (count - 1), [1] * (count - 1)
    while surplus > 0:
        candidates = [i for i in range(count - 1) if given[i] < most]
        whole, budget = sum([portions[i] for i in candidates]), surplus
        for i in candidates:
            extra = min(most - given[i], max(1, budget * portions[i] // whole), surplus)
            given[i] = given[i] + extra
            surplus = surplus - extra
    return np.array([most] + given)


def ragged_sizes(stream_key, amount, total, most, slope):
    if amount == 2:
        one = jax.random.randint(stream_key, (), max(1, total - most), min(most, total - 1) + 1)
        return jnp.stack([one, total - one])
    tallies = jnp.asarray(length_profile(amount, total, most, slope), jnp.int32)
    twos = (amount - 1) // 2
    donor, sink = tallies[1:1 + 2 * twos:2], tallies[2:2 + 2 * twos:2]
    margin = jnp.minimum(donor - 1, most - sink)
    shifted = jax.random.randint(jax.random.fold_in(stream_key, 1), (twos,), 0, 1 << 20) % (margin + 1)
    tallies = tallies.at[1:1 + 2 * twos:2].set(donor - shifted).at[2:2 + 2 * twos:2].set(sink + shifted)
    return tallies[jax.random.permutation(jax.random.fold_in(stream_key, 2), amount)]


def gaussian(rng, shape, deviation, limit, cuts=(), held_as=jnp.bfloat16):
    values = jax.random.normal(rng, shape, jnp.float32) * deviation
    if len(cuts) > 0:
        values = shard_levels(rng, shape, cuts, -0.22, 0.18) * values
    return jnp.clip(values, min=-limit, max=limit).astype(held_as)


def setup_inputs(seed: int = 0) -> dict:
    streams_of = jax.random.split(jax.random.key(seed), 9)
    return {
        "prompt_token_query": gaussian(streams_of[0], (PROMPT_TOKENS, QUERY_HEADS * HEAD_SIZE), 1.0, 6.0, ((0, 16), (1, 2))),
        "prompt_token_key": draw_prompt_token_key(jax.random.fold_in(streams_of[8], 71), 0),
        "prompt_token_value": gaussian(streams_of[2], (PROMPT_TOKENS, KEY_VALUE_HEADS * HEAD_SIZE), 1.0, 6.0, ((0, 16), (1, 2))),
        "response_query_slots": draw_response_query_slots(jax.random.fold_in(streams_of[8], 71), 0),
        "response_key_slots": gaussian(streams_of[4], (RESPONSE_TOKENS, KEY_VALUE_HEADS * HEAD_SIZE), 1.0, 6.0, ((0, 16), (1, 2))),
        "response_value_slots": gaussian(streams_of[5], (RESPONSE_TOKENS, KEY_VALUE_HEADS * HEAD_SIZE), 1.0, 6.0, ((0, 16), (1, 2))),
        "lengths": ragged_sizes(streams_of[6], MEMBERS, RESPONSE_COUNT, LONGEST_BLOCKS, 2).astype(jnp.int32),
        "block_table": jax.random.permutation(streams_of[7], RESPONSE_COUNT).astype(jnp.int32),
    }


def block_roles(lengths, global_blocks):
    bounds = jnp.cumsum(lengths).astype(jnp.int32)
    member = jnp.sum((global_blocks[:, None] >= bounds[None, :]).astype(jnp.int32), axis=1).astype(jnp.int32)
    starts = (bounds - lengths).astype(jnp.int32)
    owner_match = member[:, None] == jnp.arange(lengths.shape[0], dtype=jnp.int32)[None, :]
    first_block = jnp.sum(jnp.where(owner_match, starts[None, :], 0), axis=1).astype(jnp.int32)
    return member, (global_blocks - first_block).astype(jnp.int32), first_block


def attend(query_matrix, key_rows, value_rows, visible):
    scores = jnp.einsum("rjgd,sjd->rjgs", query_matrix.astype(jnp.float32), key_rows.astype(jnp.float32)) * (HEAD_SIZE ** -0.5)
    seen = visible[:, None, None, :]
    masked = jnp.where(seen, scores, -jnp.inf)
    peak_value = jnp.max(masked, axis=-1, keepdims=True)
    weights = jnp.where(seen, jnp.exp(scores - peak_value), 0.0)
    weight_total = jnp.sum(weights, axis=-1)
    rounded = weights.astype(jnp.bfloat16).astype(jnp.float32)
    mixed_sum = jnp.einsum("rjgs,sjd->rjgd", rounded, value_rows.astype(jnp.float32))
    return (mixed_sum / weight_total[..., None]).astype(jnp.bfloat16)


def reference(prompt_token_query, prompt_token_key, prompt_token_value, response_query_slots, response_key_slots, response_value_slots, lengths, block_table):
    query_group_width = QUERY_HEADS // KEY_VALUE_HEADS
    shared_prompt_keys = prompt_token_key.reshape(PROMPT_TOKENS, KEY_VALUE_HEADS, HEAD_SIZE)
    shared_prompt_values = prompt_token_value.reshape(PROMPT_TOKENS, KEY_VALUE_HEADS, HEAD_SIZE)

    def prompt_block(leading_row):
        query_matrix = lax.dynamic_slice_in_dim(prompt_token_query, leading_row, PROMPT_PER_SEQ, 0).reshape(PROMPT_PER_SEQ, KEY_VALUE_HEADS, query_group_width, HEAD_SIZE)
        query_positions = leading_row + jnp.arange(PROMPT_PER_SEQ, dtype=jnp.int32)
        visible = jnp.arange(PROMPT_TOKENS, dtype=jnp.int32)[None, :] <= query_positions[:, None]
        return attend(query_matrix, shared_prompt_keys, shared_prompt_values, visible).reshape(PROMPT_PER_SEQ, QUERY_HEADS * HEAD_SIZE)

    prompt_out = lax.map(prompt_block, jnp.arange(N_SEQ, dtype=jnp.int32) * PROMPT_PER_SEQ).reshape(PROMPT_TOKENS, QUERY_HEADS * HEAD_SIZE)

    inverse = jnp.argsort(block_table).astype(jnp.int32)
    blocked_keys = response_key_slots.reshape(RESPONSE_COUNT, RESPONSE_BLOCK, KEY_VALUE_HEADS, HEAD_SIZE)
    blocked_values = response_value_slots.reshape(RESPONSE_COUNT, RESPONSE_BLOCK, KEY_VALUE_HEADS, HEAD_SIZE)
    member, position, first_block = block_roles(lengths, block_table)

    def answer_block(slot_ordinal):
        query_matrix = lax.dynamic_slice_in_dim(response_query_slots, slot_ordinal * RESPONSE_BLOCK, RESPONSE_BLOCK, 0).reshape(RESPONSE_BLOCK, KEY_VALUE_HEADS, query_group_width, HEAD_SIZE)
        own_position = position[slot_ordinal]
        span = jnp.minimum(first_block[slot_ordinal] + jnp.arange(LONGEST_BLOCKS, dtype=jnp.int32), RESPONSE_COUNT - 1)
        window_slots = inverse[span]
        window_keys = blocked_keys[window_slots].reshape(LONGEST_BLOCKS * RESPONSE_BLOCK, KEY_VALUE_HEADS, HEAD_SIZE)
        window_values = blocked_values[window_slots].reshape(LONGEST_BLOCKS * RESPONSE_BLOCK, KEY_VALUE_HEADS, HEAD_SIZE)
        key_positions = jnp.arange(LONGEST_BLOCKS * RESPONSE_BLOCK, dtype=jnp.int32)
        query_positions = own_position * RESPONSE_BLOCK + jnp.arange(RESPONSE_BLOCK, dtype=jnp.int32)
        own_visible = key_positions[None, :] <= query_positions[:, None]
        visible = jnp.concatenate([jnp.ones((RESPONSE_BLOCK, PROMPT_TOKENS), dtype=bool), own_visible], axis=1)
        all_keys = jnp.concatenate([shared_prompt_keys, window_keys], axis=0)
        all_values = jnp.concatenate([shared_prompt_values, window_values], axis=0)
        return attend(query_matrix, all_keys, all_values, visible).reshape(RESPONSE_BLOCK, QUERY_HEADS * HEAD_SIZE)

    answer_out = lax.map(answer_block, jnp.arange(RESPONSE_COUNT, dtype=jnp.int32)).reshape(RESPONSE_TOKENS, QUERY_HEADS * HEAD_SIZE)
    return prompt_out, answer_out
```

```python
import functools
import math

import jax
import jax.numpy as jnp
from jax import lax
from jax.experimental import pallas as pl
from jax.experimental.pallas import tpu as pltpu
from jax.sharding import PartitionSpec as P

HEAD_SIZE = 128
RESPONSE_BLOCK = 192
NEG_FILL = -1e30
MESH = pl.DeviceIdType.MESH
SCALE = HEAD_SIZE ** (-0.5) * math.log2(math.e)


def nearest_first(count):
    order = []
    for step in range(1, count // 2 + 1):
        order.append(step)
        if count - step != step:
            order.append(count - step)
    return order


def softmax_step(state, scores, value_rows):
    peak = jnp.max(scores, axis=-1, keepdims=True)
    if state is not None:
        peak = jnp.maximum(state[0], peak)
    weights = jnp.exp2(scores - peak)
    total = jnp.sum(weights, axis=-1, keepdims=True)
    mixed = jnp.dot(weights.astype(jnp.bfloat16), value_rows, preferred_element_type=jnp.float32)
    if state is not None:
        factor = jnp.exp2(state[0] - peak)
        total = state[1] * factor + total
        mixed = state[2] * factor + mixed
    return (peak, total, mixed)


def score(query_rows, key_rows):
    return (
        lax.dot_general(
            query_rows, key_rows, (((1,), (1,)), ((), ())), preferred_element_type=jnp.float32
        )
        * SCALE
    )


def kernel(
    seq_count, head_count, heads_kv, group, most, chunk,
    lengths_ref, table_ref, pq_hbm, pk_hbm, pv_hbm, rq_hbm, rk_hbm, rv_hbm,
    pout_ref, aout_ref,
    *scratch,
):
    pieces = scratch[:heads_kv]
    stage_a = scratch[heads_kv:2 * heads_kv]
    stage_p = scratch[2 * heads_kv:3 * heads_kv]
    (keys, values, queries, pqueries, pack_sem, q_sem, recv_sem, z_sem, x_sem, c_sem,
     out_send, out_recv, out_local) = scratch[3 * heads_kv:]
    prompt_rows = pq_hbm.shape[0]
    block = rq_hbm.shape[0]
    prompt_total = prompt_rows * seq_count
    width = group * HEAD_SIZE
    z_count = seq_count // 4
    me = lax.axis_index("seq")
    head = lax.axis_index("head")
    z, x, c = me // 4, (me // 2) % 2, me % 2

    def place(zi, xi, ci):
        return zi * 4 + xi * 2 + ci

    x_peer, c_peer = place(z, 1 - x, c), place(z, x, 1 - c)
    offsets = nearest_first(z_count)

    packs = []
    for j in range(heads_kv):
        cols = pl.ds(j * HEAD_SIZE, HEAD_SIZE)
        row = 0
        for k, source in enumerate((rk_hbm, rv_hbm, pk_hbm, pv_hbm)):
            rows = source.shape[0]
            copy = pltpu.make_async_copy(
                source.at[:, cols], pieces[j].at[me, pl.ds(row, rows), :], pack_sem.at[j, k]
            )
            copy.start()
            packs.append(copy)
            row += rows
    q_copies = [
        pltpu.make_async_copy(rq_hbm, queries, q_sem.at[0]),
        pltpu.make_async_copy(pq_hbm, pqueries, q_sem.at[1]),
    ]
    for copy in q_copies:
        copy.start()

    barrier = pltpu.get_barrier_semaphore()
    peers = [(place((z + k) % z_count, x, c), head) for k in range(1, z_count)]
    peers += [(x_peer, head), (c_peer, head)]
    peers += [(me, (head + k) % head_count) for k in range(1, head_count)]
    for peer in peers:
        pl.semaphore_signal(barrier, inc=1, device_id=peer, device_id_type=MESH)
    pl.semaphore_wait(barrier, len(peers))

    sends = []

    def send(j, source, target, sem):
        copy = pltpu.make_async_remote_copy(
            src_ref=pieces[j].at[source], dst_ref=pieces[j].at[source],
            send_sem=sem, recv_sem=recv_sem.at[j, source],
            device_id=(target, head), device_id_type=MESH,
        )
        copy.start()
        sends.append((j, copy))

    def arrived(j, source):
        pltpu.make_async_remote_copy(
            src_ref=pieces[j].at[source], dst_ref=pieces[j].at[source],
            send_sem=c_sem.at[j, 0, 0], recv_sem=recv_sem.at[j, source],
            device_id=(c_peer, head), device_id_type=MESH,
        ).wait_recv()

    def x_own(j):
        if j < heads_kv:
            send(j, me, x_peer, x_sem.at[j, 0])

    def forward_z(j, k):
        if j < heads_kv:
            source = place((z + z_count - offsets[k]) % z_count, x, c)
            arrived(j, source)
            send(j, source, x_peer, x_sem.at[j, offsets[k]])
            send(j, source, c_peer, c_sem.at[j, 0, offsets[k]])

    def forward_x(j):
        if j < heads_kv:
            for k in [0] + offsets:
                source = place((z + z_count - k) % z_count, 1 - x, c)
                arrived(j, source)
                send(j, source, c_peer, c_sem.at[j, 1, k])

    def wait_c(j):
        for xi in range(2):
            for zi in range(z_count):
                arrived(j, place(zi, xi, 1 - c))

    for j in range(heads_kv):
        for copy in packs[4 * j:4 * j + 4]:
            copy.wait()
        for k in offsets:
            send(j, me, place((z + k) % z_count, x, c), z_sem.at[j, k])
        if j == 0:
            x_own(0)
        send(j, me, c_peer, c_sem.at[j, 0, 0])
    x_own(1)

    own = table_ref[me]
    first = jnp.int32(0)
    bound = jnp.int32(0)
    for m in range(lengths_ref.shape[0]):
        bound = bound + lengths_ref[m]
        first = jnp.where(own >= bound, bound, first)
    base = prompt_total + (own - first) * block
    slots = []
    for p in range(most):
        wanted = first + p
        slots.append(
            lax.fori_loop(
                0, seq_count,
                lambda s, a, wanted=wanted: jnp.where(table_ref[s] == wanted, s, a),
                jnp.int32(0),
            )
        )

    for k in range(len(offsets)):
        forward_z(0, k)
    forward_x(0)
    for copy in q_copies:
        copy.wait()

    total_keys = prompt_total + most * block
    bounds = [(0, prompt_total)]
    at = prompt_total
    while at < total_keys:
        bounds.append((at, min(chunk, total_keys - at)))
        at += bounds[-1][1]
    pair = 2
    steps = group // pair
    out_copies = []

    for j in range(heads_kv):
        wait_c(j)
        for s in range(seq_count):
            rows = pl.ds(s * prompt_rows, prompt_rows)
            keys[rows, :] = pieces[j][s, 2 * block:2 * block + prompt_rows, :]
            values[rows, :] = pieces[j][s, 2 * block + prompt_rows:2 * (block + prompt_rows), :]
        for p in range(most):
            rows = pl.ds(prompt_total + p * block, block)
            keys[rows, :] = pieces[j][slots[p], 0:block, :]
            values[rows, :] = pieces[j][slots[p], block:2 * block, :]

        query = jnp.concatenate(
            [pqueries[:, (j * group + g) * HEAD_SIZE:(j * group + g + 1) * HEAD_SIZE] for g in range(group)],
            axis=0,
        )
        scores = score(query, keys[0:prompt_total, :])
        key_at = lax.broadcasted_iota(jnp.int32, scores.shape, 1)
        query_at = me * prompt_rows + lax.broadcasted_iota(jnp.int32, scores.shape, 0) % prompt_rows
        scores = jnp.where(key_at <= query_at, scores, NEG_FILL)
        state = softmax_step(None, scores, values[0:prompt_total, :])
        out = (state[2] / state[1]).astype(jnp.bfloat16)
        part = prompt_rows // head_count
        for g in range(group):
            for h in range(head_count):
                stage_p[j][h, :, g * HEAD_SIZE:(g + 1) * HEAD_SIZE] = out[
                    g * prompt_rows + h * part:g * prompt_rows + (h + 1) * part, :
                ]

        def step(i, carry, j=j):
            for k in range(len(offsets)):
                if k < steps - 1:
                    last = len(offsets) if k == steps - 2 else k + 1

                    @pl.when(i == k + 1)
                    def _(k=k, last=last):
                        for kk in range(k, last):
                            forward_z(j + 1, kk)
                        if k == min(len(offsets), steps - 1) - 1:
                            x_own(j + 2)
            states = [None] * pair
            rows_of = []
            for u in range(pair):
                cols = pl.ds(pl.multiple_of((j * group + i * pair + u) * HEAD_SIZE, HEAD_SIZE), HEAD_SIZE)
                rows_of.append(queries[:, cols])
            for n, (start, size) in enumerate(bounds):
                for u in range(pair):
                    scores = score(rows_of[u], keys[start:start + size, :])
                    if start >= prompt_total:
                        gap = lax.broadcasted_iota(jnp.int32, scores.shape, 1) - lax.broadcasted_iota(
                            jnp.int32, scores.shape, 0
                        )
                        scores = jnp.where(gap <= base - start, scores, NEG_FILL)
                    states[u] = softmax_step(states[u], scores, values[start:start + size, :])
            share = block // head_count
            for u in range(pair):
                out = (states[u][2] / states[u][1]).astype(jnp.bfloat16)
                cols = pl.ds(pl.multiple_of((i * pair + u) * HEAD_SIZE, HEAD_SIZE), HEAD_SIZE)
                for h in range(head_count):
                    stage_a[j][h, :, cols] = out[h * share:(h + 1) * share, :]
            return carry

        lax.fori_loop(0, steps, step, 0)
        forward_x(j + 1)

        cols = pl.ds(pl.multiple_of((head * heads_kv + j) * width, width), width)
        for n, (staged, result) in enumerate(((stage_a[j], aout_ref), (stage_p[j], pout_ref))):
            for k in range(1, head_count):
                target = (head + k) % head_count
                copy = pltpu.make_async_remote_copy(
                    src_ref=staged.at[target], dst_ref=result.at[:, cols],
                    send_sem=out_send.at[j, n, k], recv_sem=out_recv.at[j, n, head],
                    device_id=(me, target), device_id_type=MESH,
                )
                copy.start()
                sends.append((j, copy))
            local = pltpu.make_async_copy(staged.at[head], result.at[:, cols], out_local.at[j, n])
            local.start()
            out_copies.append(local)

    for local in out_copies:
        local.wait()
    for j in range(heads_kv):
        for k in range(1, head_count):
            other = (head + k) % head_count
            cols = pl.ds(pl.multiple_of((other * heads_kv + j) * width, width), width)
            for n, (staged, result) in enumerate(((stage_a[j], aout_ref), (stage_p[j], pout_ref))):
                pltpu.make_async_remote_copy(
                    src_ref=staged.at[other], dst_ref=result.at[:, cols],
                    send_sem=out_send.at[j, n, k], recv_sem=out_recv.at[j, n, other],
                    device_id=(me, other), device_id_type=MESH,
                ).wait_recv()
    for j in range(heads_kv):
        for k in offsets:
            wait_sent(pieces[j].at[me], z_sem.at[j, k], c_peer, head)
        for k in range(z_count):
            wait_sent(pieces[j].at[me], x_sem.at[j, k], c_peer, head)
            for n in range(2):
                wait_sent(pieces[j].at[me], c_sem.at[j, n, k], c_peer, head)
        for n, staged in enumerate((stage_a[j], stage_p[j])):
            for k in range(1, head_count):
                wait_sent(staged.at[0], out_send.at[j, n, k], c_peer, head)


def wait_sent(ref, sem, peer, head):
    pltpu.make_async_remote_copy(
        src_ref=ref, dst_ref=ref, send_sem=sem, recv_sem=sem,
        device_id=(peer, head), device_id_type=MESH,
    ).wait_send()


def on_device(mesh_shape, pq, pk, pv, rq, rk, rv, lengths, table):
    seq_count, head_count = mesh_shape["seq"], mesh_shape["head"]
    heads_kv = rk.shape[1] // HEAD_SIZE
    group = rq.shape[1] // rk.shape[1]
    block, prompt_rows = rq.shape[0], pq.shape[0]
    most = table.shape[0] // 2
    width = group * HEAD_SIZE
    z_count = seq_count // 4
    total = prompt_rows * seq_count + most * block
    dma = pltpu.SemaphoreType.DMA
    any_space = pl.BlockSpec(memory_space=pl.ANY)
    smem = pl.BlockSpec(memory_space=pltpu.SMEM)
    vmem = pl.BlockSpec(memory_space=pltpu.VMEM)
    return pl.pallas_call(
        functools.partial(kernel, seq_count, head_count, heads_kv, group, most, 512),
        out_shape=(
            jax.ShapeDtypeStruct((prompt_rows // head_count, rq.shape[1] * head_count), jnp.bfloat16),
            jax.ShapeDtypeStruct((block // head_count, rq.shape[1] * head_count), jnp.bfloat16),
        ),
        in_specs=[smem] * 2 + [any_space] * 6,
        out_specs=(vmem, vmem),
        scratch_shapes=(
            [pltpu.VMEM((seq_count, 2 * (block + prompt_rows), HEAD_SIZE), jnp.bfloat16)] * heads_kv
            + [pltpu.VMEM((head_count, block // head_count, width), jnp.bfloat16)] * heads_kv
            + [pltpu.VMEM((head_count, prompt_rows // head_count, width), jnp.bfloat16)] * heads_kv
            + [
                pltpu.VMEM((total, HEAD_SIZE), jnp.bfloat16),
                pltpu.VMEM((total, HEAD_SIZE), jnp.bfloat16),
                pltpu.VMEM(rq.shape, jnp.bfloat16),
                pltpu.VMEM(pq.shape, jnp.bfloat16),
                dma((heads_kv, 4)),
                dma((2,)),
                dma((heads_kv, seq_count)),
                dma((heads_kv, z_count)),
                dma((heads_kv, z_count)),
                dma((heads_kv, 2, z_count)),
                dma((heads_kv, 2, head_count)),
                dma((heads_kv, 2, head_count)),
                dma((heads_kv, 2)),
            ]
        ),
        compiler_params=pltpu.CompilerParams(
            collective_id=0, has_side_effects=True, vmem_limit_bytes=60 * 1024 * 1024
        ),
    )(lengths, table, pq, pk, pv, rq, rk, rv)


def solution(mesh):
    sharded = P("seq", "head")
    out = P(("seq", "head"), None)
    return jax.shard_map(
        functools.partial(on_device, dict(mesh.shape)), mesh=mesh,
        in_specs=(sharded,) * 6 + (P(), P()), out_specs=(out, out), check_vma=False,
    )
```

```python
import functools
import math

import jax
import jax.numpy as jnp
from jax import lax
from jax.experimental import pallas as pl
from jax.experimental.pallas import tpu as pltpu
from jax.sharding import PartitionSpec as P

HEAD_SIZE = 128
RESPONSE_BLOCK = 192
NEG_FILL = -1e30
MESH = pl.DeviceIdType.MESH
SCALE = HEAD_SIZE ** (-0.5) * math.log2(math.e)


def nearest_first(count):
    order = []
    for step in range(1, count // 2 + 1):
        order.append(step)
        if count - step != step:
            order.append(count - step)
    return order


def softmax_step(state, scores, value_rows):
    peak = jnp.max(scores, axis=-1, keepdims=True)
    if state is not None:
        peak = jnp.maximum(state[0], peak)
    weights = jnp.exp2(scores - peak)
    total = jnp.sum(weights, axis=-1, keepdims=True)
    mixed = jnp.dot(weights.astype(jnp.bfloat16), value_rows, preferred_element_type=jnp.float32)
    if state is not None:
        factor = jnp.exp2(state[0] - peak)
        total = state[1] * factor + total
        mixed = state[2] * factor + mixed
    return (peak, total, mixed)


def score(query_rows, key_rows):
    return (
        lax.dot_general(
            query_rows, key_rows, (((1,), (1,)), ((), ())), preferred_element_type=jnp.float32
        )
        * SCALE
    )


def kernel(
    seq_count, head_count, heads_kv, group, most, chunk,
    lengths_ref, table_ref, pq_hbm, pk_hbm, pv_hbm, rq_hbm, rk_hbm, rv_hbm,
    pout_ref, aout_ref,
    *scratch,
):
    pieces = scratch[:heads_kv]
    stage_a = scratch[heads_kv:2 * heads_kv]
    stage_p = scratch[2 * heads_kv:3 * heads_kv]
    (keys, values, queries, pqueries, pack_sem, q_sem, recv_sem, z_sem, x_sem, c_sem,
     out_send, out_recv, out_local, bias, *rest) = scratch[3 * heads_kv:]
    score_bufs, peaks = rest[:2], rest[2:]
    prompt_rows = pq_hbm.shape[0]
    block = rq_hbm.shape[0]
    prompt_total = prompt_rows * seq_count
    width = group * HEAD_SIZE
    z_count = seq_count // 4
    me = lax.axis_index("seq")
    head = lax.axis_index("head")
    z, x, c = me // 4, (me // 2) % 2, me % 2

    def z_source_offset(k):
        if relayed:
            return (z + 4 - z_source(k)) % 4
        return offsets[k]

    def place(zi, xi, ci):
        return zi * 4 + xi * 2 + ci

    x_peer, c_peer = place(z, 1 - x, c), place(z, x, 1 - c)
    offsets = nearest_first(z_count)
    relayed = z_count == 4
    inner = jnp.where((z == 1) | (z == 2), 1, 0)

    def mirrored(t):
        return jnp.where(z < 2, t, 3 - t)

    def z_source(k):
        if relayed:
            return mirrored((inner + 1 + k) % 4)
        return (z + z_count - offsets[k]) % z_count


    packs = []
    for j in range(heads_kv):
        cols = pl.ds(j * HEAD_SIZE, HEAD_SIZE)
        row = 0
        for k, source in enumerate((rk_hbm, rv_hbm, pk_hbm, pv_hbm)):
            rows = source.shape[0]
            copy = pltpu.make_async_copy(
                source.at[:, cols], pieces[j].at[me, pl.ds(row, rows), :], pack_sem.at[j, k]
            )
            copy.start()
            packs.append(copy)
            row += rows
    q_copies = [
        pltpu.make_async_copy(rq_hbm, queries, q_sem.at[0]),
        pltpu.make_async_copy(pq_hbm, pqueries, q_sem.at[1]),
    ]
    for copy in q_copies:
        copy.start()

    barrier = pltpu.get_barrier_semaphore()
    peers = [(place((z + k) % z_count, x, c), head) for k in range(1, z_count)]
    peers += [(x_peer, head), (c_peer, head)]
    peers += [(me, (head + k) % head_count) for k in range(1, head_count)]
    for peer in peers:
        pl.semaphore_signal(barrier, inc=1, device_id=peer, device_id_type=MESH)
    pl.semaphore_wait(barrier, len(peers))

    sends = []

    def send(j, source, target, sem):
        copy = pltpu.make_async_remote_copy(
            src_ref=pieces[j].at[source], dst_ref=pieces[j].at[source],
            send_sem=sem, recv_sem=recv_sem.at[j, source],
            device_id=(target, head), device_id_type=MESH,
        )
        copy.start()
        sends.append((j, copy))

    def arrived(j, source):
        pltpu.make_async_remote_copy(
            src_ref=pieces[j].at[source], dst_ref=pieces[j].at[source],
            send_sem=c_sem.at[j, 0, 0], recv_sem=recv_sem.at[j, source],
            device_id=(c_peer, head), device_id_type=MESH,
        ).wait_recv()

    def x_own(j):
        if j < heads_kv:
            send(j, me, x_peer, x_sem.at[j, 0])

    def forward_z(j, k):
        if j < heads_kv:
            source = place(z_source(k), x, c)
            arrived(j, source)
            if relayed and k < 2:
                @pl.when(inner == 1)
                def _():
                    send(j, source, place(mirrored(0), x, c), z_sem.at[j, 2 + k])
            send(j, source, x_peer, x_sem.at[j, offsets[k]])
            send(j, source, c_peer, c_sem.at[j, 0, offsets[k]])

    def forward_x(j, half):
        if j < heads_kv:
            arrivals = [0] + [z_source_offset(k) for k in range(len(offsets))]
            for k in arrivals[:len(arrivals) // 2] if half == 0 else arrivals[len(arrivals) // 2:]:
                source = place((z + z_count - k) % z_count, 1 - x, c)
                arrived(j, source)
                send(j, source, c_peer, c_sem.at[j, 1, k])

    def wait_c(j):
        for xi in range(2):
            for zi in range(z_count):
                arrived(j, place(zi, xi, 1 - c))

    for j in range(heads_kv):
        for copy in packs[4 * j:4 * j + 4]:
            copy.wait()
        if relayed:
            send(j, me, place(mirrored(1 - inner), x, c), z_sem.at[j, 0])
            send(j, me, place(mirrored(2), x, c), z_sem.at[j, 1])
        else:
            for k in offsets:
                send(j, me, place((z + k) % z_count, x, c), z_sem.at[j, k])
        if j == 0:
            x_own(0)
        send(j, me, c_peer, c_sem.at[j, 0, 0])

    own = table_ref[me]
    first = jnp.int32(0)
    bound = jnp.int32(0)
    for m in range(lengths_ref.shape[0]):
        bound = bound + lengths_ref[m]
        first = jnp.where(own >= bound, bound, first)
    slots = []
    for p in range(most):
        wanted = first + p
        slots.append(
            lax.fori_loop(
                0, seq_count,
                lambda s, a, wanted=wanted: jnp.where(table_ref[s] == wanted, s, a),
                jnp.int32(0),
            )
        )

    for start in range(0, most * block, block):
        gap = lax.broadcasted_iota(jnp.int32, (block, block), 1) - lax.broadcasted_iota(
            jnp.int32, (block, block), 0
        )
        bias[:, start:start + block] = jnp.where(gap <= (own - first) * block - start, 0.0, NEG_FILL)
    for k in range(len(offsets)):
        forward_z(0, k)
    x_own(1)
    forward_x(0, 0)
    forward_x(0, 1)
    for copy in q_copies:
        copy.wait()

    total_keys = prompt_total + most * block
    bounds = [(0, prompt_total)]
    at = prompt_total
    while at < total_keys:
        bounds.append((at, min(chunk, total_keys - at)))
        at += bounds[-1][1]
    pair = 2
    steps = group // pair

    part_width = pair * HEAD_SIZE

    def out_refs(j, i, owner):
        wide = part_width
        if isinstance(i, int) and i == steps:
            staged, result, start, wide = stage_p[j], pout_ref, 0, width
        else:
            staged, result, start = stage_a[j], aout_ref, i * part_width
        start = start if isinstance(start, int) else pl.multiple_of(start, part_width)
        cols = pl.ds(pl.multiple_of((owner * heads_kv + j) * width + start, wide), wide)
        return staged, result.at[:, cols], pl.ds(start, wide)

    def out_remote(j, i, k, owner):
        target = (head + k) % head_count
        staged, result, cols = out_refs(j, i, owner)
        return pltpu.make_async_remote_copy(
            src_ref=staged.at[target, :, cols], dst_ref=result,
            send_sem=out_send.at[j, i, k], recv_sem=out_recv.at[j, i, owner],
            device_id=(me, target), device_id_type=MESH,
        )

    def out_copy(j, i):
        staged, result, cols = out_refs(j, i, head)
        return pltpu.make_async_copy(staged.at[head, :, cols], result, out_local.at[j, i])

    def send_out(j, i):
        for k in range(1, head_count):
            out_remote(j, i, k, head).start()
        out_copy(j, i).start()

    for j in range(heads_kv):
        wait_c(j)
        for s in range(seq_count):
            rows = pl.ds(s * prompt_rows, prompt_rows)
            keys[rows, :] = pieces[j][s, 2 * block:2 * block + prompt_rows, :]
            values[rows, :] = pieces[j][s, 2 * block + prompt_rows:2 * (block + prompt_rows), :]
        for p in range(most):
            rows = pl.ds(prompt_total + p * block, block)
            keys[rows, :] = pieces[j][slots[p], 0:block, :]
            values[rows, :] = pieces[j][slots[p], block:2 * block, :]

        query = jnp.concatenate(
            [pqueries[:, (j * group + g) * HEAD_SIZE:(j * group + g + 1) * HEAD_SIZE] for g in range(group)],
            axis=0,
        )
        scores = score(query, keys[0:prompt_total, :])
        key_at = lax.broadcasted_iota(jnp.int32, scores.shape, 1)
        query_at = me * prompt_rows + lax.broadcasted_iota(jnp.int32, scores.shape, 0) % prompt_rows
        scores = jnp.where(key_at <= query_at, scores, NEG_FILL)
        state = softmax_step(None, scores, values[0:prompt_total, :])
        out = (state[2] / state[1]).astype(jnp.bfloat16)
        part = prompt_rows // head_count
        for g in range(group):
            for h in range(head_count):
                stage_p[j][h, :, g * HEAD_SIZE:(g + 1) * HEAD_SIZE] = out[
                    g * prompt_rows + h * part:g * prompt_rows + (h + 1) * part, :
                ]

        def first_pass(g, u):
            cols = pl.ds(pl.multiple_of((j * group + g) * HEAD_SIZE, HEAD_SIZE), HEAD_SIZE)
            query = queries[:, cols]
            peak = None
            for start, size in bounds:
                raw = lax.dot_general(
                    query, keys[start:start + size, :], (((1,), (1,)), ((), ())),
                    preferred_element_type=jnp.float32,
                )
                if start >= prompt_total:
                    raw = raw + bias[:, start - prompt_total:start - prompt_total + size]
                score_bufs[u][:, start:start + size] = raw
                for lane in range(0, size, HEAD_SIZE):
                    strip = raw[:, lane:lane + HEAD_SIZE]
                    peak = strip if peak is None else jnp.maximum(peak, strip)
            peaks[u][...] = peak

        def second_pass(g, u):
            peak = jnp.max(peaks[u][...], axis=-1, keepdims=True) * SCALE
            total = mixed = None
            for start, size in bounds:
                weights = jnp.exp2(score_bufs[u][:, start:start + size] * SCALE - peak)
                for lane in range(0, size, HEAD_SIZE):
                    strip = weights[:, lane:lane + HEAD_SIZE]
                    total = strip if total is None else total + strip
                part = jnp.dot(
                    weights.astype(jnp.bfloat16), values[start:start + size, :],
                    preferred_element_type=jnp.float32,
                )
                mixed = part if mixed is None else mixed + part
            out = (mixed / jnp.sum(total, axis=-1, keepdims=True)).astype(jnp.bfloat16)
            cols = pl.ds(pl.multiple_of(g * HEAD_SIZE, HEAD_SIZE), HEAD_SIZE)
            share = block // head_count
            for h in range(head_count):
                stage_a[j][h, :, cols] = out[h * share:(h + 1) * share, :]

        def hooks(i):
            @pl.when(i == 0)
            def _():
                send_out(j, steps)

            @pl.when(i > 0)
            def _():
                send_out(j, i - 1)

            third = -(-len(offsets) // 3)
            everything = list(range(len(offsets)))
            plan = [[] for _ in range(steps)]
            if j == 0:
                plan[0] += [(1, k) for k in everything] + [(2, None)]
                plan[1] += [(2, k) for k in everything[:third]]
                plan[2] += [(2, k) for k in everything[third:2 * third]]
            elif j == 1:
                plan[0] += [(2, k) for k in everything[2 * third:]] + [(3, None)]
            if j > 0:
                plan[1] += [(j + 2, k) for k in everything[:third]]
                plan[2] += [(j + 2, k) for k in everything[third:]] + [(j + 3, None)]
            for at, actions in enumerate(plan):
                @pl.when(i == at)
                def _(at=at, actions=actions):
                    for target, k in actions:
                        if k is None:
                            x_own(target)
                        else:
                            forward_z(target, k)
                    if at >= steps - 2:
                        forward_x(j + 1, at - (steps - 2))

        def step(i, carry):
            first_pass(2 * i + 1, 1)
            second_pass(2 * i, 0)
            first_pass(jnp.minimum(2 * i + 2, group - 1), 0)
            second_pass(2 * i + 1, 1)
            hooks(i)
            return carry

        first_pass(0, 0)
        lax.fori_loop(0, steps, step, 0)

        send_out(j, steps - 1)

    def out_parts():
        for j in range(heads_kv):
            for i in range(steps + 1):
                yield j, i

    for j, i in out_parts():
        out_copy(j, i).wait()
    for j, i in out_parts():
        for k in range(1, head_count):
            out_remote(j, i, k, (head + k) % head_count).wait_recv()
    for j in range(heads_kv):
        if relayed:
            for k in range(2):
                wait_sent(pieces[j].at[me], z_sem.at[j, k], c_peer, head)

            @pl.when(inner == 1)
            def _(j=j):
                for k in range(2):
                    wait_sent(pieces[j].at[me], z_sem.at[j, 2 + k], c_peer, head)
        else:
            for k in offsets:
                wait_sent(pieces[j].at[me], z_sem.at[j, k], c_peer, head)
        for k in range(z_count):
            wait_sent(pieces[j].at[me], x_sem.at[j, k], c_peer, head)
            for n in range(2):
                wait_sent(pieces[j].at[me], c_sem.at[j, n, k], c_peer, head)
    for j, i in out_parts():
        for k in range(1, head_count):
            out_remote(j, i, k, (head + k) % head_count).wait_send()


def wait_sent(ref, sem, peer, head):
    pltpu.make_async_remote_copy(
        src_ref=ref, dst_ref=ref, send_sem=sem, recv_sem=sem,
        device_id=(peer, head), device_id_type=MESH,
    ).wait_send()


def on_device(mesh_shape, pq, pk, pv, rq, rk, rv, lengths, table):
    seq_count, head_count = mesh_shape["seq"], mesh_shape["head"]
    heads_kv = rk.shape[1] // HEAD_SIZE
    group = rq.shape[1] // rk.shape[1]
    block, prompt_rows = rq.shape[0], pq.shape[0]
    most = table.shape[0] // 2
    width = group * HEAD_SIZE
    z_count = seq_count // 4
    total = prompt_rows * seq_count + most * block
    dma = pltpu.SemaphoreType.DMA
    any_space = pl.BlockSpec(memory_space=pl.ANY)
    smem = pl.BlockSpec(memory_space=pltpu.SMEM)
    return pl.pallas_call(
        functools.partial(kernel, seq_count, head_count, heads_kv, group, most, 512),
        out_shape=(
            jax.ShapeDtypeStruct((prompt_rows // head_count, rq.shape[1] * head_count), jnp.bfloat16),
            jax.ShapeDtypeStruct((block // head_count, rq.shape[1] * head_count), jnp.bfloat16),
        ),
        in_specs=[smem] * 2 + [any_space] * 6,
        out_specs=(any_space, any_space),
        scratch_shapes=(
            [pltpu.VMEM((seq_count, 2 * (block + prompt_rows), HEAD_SIZE), jnp.bfloat16)] * heads_kv
            + [pltpu.VMEM((head_count, block // head_count, width), jnp.bfloat16)] * heads_kv
            + [pltpu.VMEM((head_count, prompt_rows // head_count, width), jnp.bfloat16)] * heads_kv
            + [
                pltpu.VMEM((total, HEAD_SIZE), jnp.bfloat16),
                pltpu.VMEM((total, HEAD_SIZE), jnp.bfloat16),
                pltpu.VMEM(rq.shape, jnp.bfloat16),
                pltpu.VMEM(pq.shape, jnp.bfloat16),
                dma((heads_kv, 4)),
                dma((2,)),
                dma((heads_kv, seq_count)),
                dma((heads_kv, max(z_count, 4))),
                dma((heads_kv, z_count)),
                dma((heads_kv, 2, z_count)),
                dma((heads_kv, group // 2 + 1, head_count)),
                dma((heads_kv, group // 2 + 1, head_count)),
                dma((heads_kv, group // 2 + 1)),
                pltpu.VMEM((block, most * block), jnp.float32),
            ]
            + [pltpu.VMEM((block, total), jnp.float32)] * 2
            + [pltpu.VMEM((block, HEAD_SIZE), jnp.float32)] * 2
        ),
        compiler_params=pltpu.CompilerParams(
            collective_id=0, has_side_effects=True, vmem_limit_bytes=60 * 1024 * 1024
        ),
    )(lengths, table, pq, pk, pv, rq, rk, rv)


def solution(mesh):
    sharded = P("seq", "head")
    out = P(("seq", "head"), None)
    return jax.shard_map(
        functools.partial(on_device, dict(mesh.shape)), mesh=mesh,
        in_specs=(sharded,) * 6 + (P(), P()), out_specs=(out, out), check_vma=False,
    )
```

```python
import functools
import math

import jax
import jax.numpy as jnp
from jax import lax
from jax.experimental import pallas as pl
from jax.experimental.pallas import tpu as pltpu
from jax.sharding import PartitionSpec as P

HEAD_SIZE = 128
RESPONSE_BLOCK = 192
NEG_FILL = -1e30
MESH = pl.DeviceIdType.MESH
SCALE = HEAD_SIZE ** (-0.5) * math.log2(math.e)


def nearest_first(count):
    order = []
    for step in range(1, count // 2 + 1):
        order.append(step)
        if count - step != step:
            order.append(count - step)
    return order


def softmax_step(state, scores, value_rows):
    peak = jnp.max(scores, axis=-1, keepdims=True)
    if state is not None:
        peak = jnp.maximum(state[0], peak)
    weights = jnp.exp2(scores - peak)
    total = jnp.sum(weights, axis=-1, keepdims=True)
    mixed = jnp.dot(weights.astype(jnp.bfloat16), value_rows, preferred_element_type=jnp.float32)
    if state is not None:
        factor = jnp.exp2(state[0] - peak)
        total = state[1] * factor + total
        mixed = state[2] * factor + mixed
    return (peak, total, mixed)


def score(query_rows, key_rows):
    return (
        lax.dot_general(
            query_rows, key_rows, (((1,), (1,)), ((), ())), preferred_element_type=jnp.float32
        )
        * SCALE
    )


def kernel(
    seq_count, head_count, heads_kv, group, most, chunk,
    lengths_ref, table_ref, pq_hbm, pk_hbm, pv_hbm, rq_hbm, rk_hbm, rv_hbm,
    pout_ref, aout_ref,
    *scratch,
):
    pieces = scratch[:heads_kv]
    stage_a = scratch[heads_kv:2 * heads_kv]
    stage_p = scratch[2 * heads_kv:3 * heads_kv]
    (keys, values, queries, pqueries, pack_sem, q_sem, recv_sem, z_sem, x_sem, c_sem,
     out_send, out_recv, out_local, bias, *rest) = scratch[3 * heads_kv:]
    score_bufs, peaks = rest[:2], rest[2:]
    prompt_rows = pq_hbm.shape[0]
    block = rq_hbm.shape[0]
    prompt_total = prompt_rows * seq_count
    width = group * HEAD_SIZE
    z_count = seq_count // 4
    me = lax.axis_index("seq")
    head = lax.axis_index("head")
    z, x, c = me // 4, (me // 2) % 2, me % 2

    def z_source_offset(k):
        if relayed:
            return (z + 4 - z_source(k)) % 4
        return offsets[k]

    def place(zi, xi, ci):
        return zi * 4 + xi * 2 + ci

    x_peer, c_peer = place(z, 1 - x, c), place(z, x, 1 - c)
    offsets = nearest_first(z_count)
    relayed = z_count == 4
    inner = jnp.where((z == 1) | (z == 2), 1, 0)

    def mirrored(t):
        return jnp.where(z < 2, t, 3 - t)

    def z_source(k):
        if relayed:
            return mirrored((inner + 1 + k) % 4)
        return (z + z_count - offsets[k]) % z_count


    packs = []
    for j in range(heads_kv):
        cols = pl.ds(j * HEAD_SIZE, HEAD_SIZE)
        row = 0
        for k, source in enumerate((rk_hbm, rv_hbm, pk_hbm, pv_hbm)):
            rows = source.shape[0]
            copy = pltpu.make_async_copy(
                source.at[:, cols], pieces[j].at[me, pl.ds(row, rows), :], pack_sem.at[j, k]
            )
            copy.start()
            packs.append(copy)
            row += rows
    q_copies = [
        pltpu.make_async_copy(rq_hbm, queries, q_sem.at[0]),
        pltpu.make_async_copy(pq_hbm, pqueries, q_sem.at[1]),
    ]
    for copy in q_copies:
        copy.start()

    barrier = pltpu.get_barrier_semaphore()
    peers = [(place((z + k) % z_count, x, c), head) for k in range(1, z_count)]
    peers += [(x_peer, head), (c_peer, head)]
    peers += [(me, (head + k) % head_count) for k in range(1, head_count)]
    for peer in peers:
        pl.semaphore_signal(barrier, inc=1, device_id=peer, device_id_type=MESH)
    pl.semaphore_wait(barrier, len(peers))

    sends = []

    def send(j, source, target, sem):
        copy = pltpu.make_async_remote_copy(
            src_ref=pieces[j].at[source], dst_ref=pieces[j].at[source],
            send_sem=sem, recv_sem=recv_sem.at[j, source],
            device_id=(target, head), device_id_type=MESH,
        )
        copy.start()
        sends.append((j, copy))

    def arrived(j, source):
        pltpu.make_async_remote_copy(
            src_ref=pieces[j].at[source], dst_ref=pieces[j].at[source],
            send_sem=c_sem.at[j, 0, 0], recv_sem=recv_sem.at[j, source],
            device_id=(c_peer, head), device_id_type=MESH,
        ).wait_recv()

    def x_own(j):
        if j < heads_kv:
            send(j, me, x_peer, x_sem.at[j, 0])

    def forward_z(j, k):
        if j < heads_kv:
            source = place(z_source(k), x, c)
            arrived(j, source)
            if relayed and k < 2:
                @pl.when(inner == 1)
                def _():
                    send(j, source, place(mirrored(0), x, c), z_sem.at[j, 2 + k])
            send(j, source, x_peer, x_sem.at[j, offsets[k]])
            send(j, source, c_peer, c_sem.at[j, 0, offsets[k]])

    def forward_x(j, half):
        if j < heads_kv:
            arrivals = [0] + [z_source_offset(k) for k in range(len(offsets))]
            for k in arrivals[:len(arrivals) // 2] if half == 0 else arrivals[len(arrivals) // 2:]:
                source = place((z + z_count - k) % z_count, 1 - x, c)
                arrived(j, source)
                send(j, source, c_peer, c_sem.at[j, 1, k])

    def wait_c(j):
        for xi in range(2):
            for zi in range(z_count):
                arrived(j, place(zi, xi, 1 - c))

    for j in range(heads_kv):
        for copy in packs[4 * j:4 * j + 4]:
            copy.wait()
        if relayed:
            send(j, me, place(mirrored(1 - inner), x, c), z_sem.at[j, 0])
            send(j, me, place(mirrored(2), x, c), z_sem.at[j, 1])
        else:
            for k in offsets:
                send(j, me, place((z + k) % z_count, x, c), z_sem.at[j, k])
        if j == 0:
            x_own(0)
        send(j, me, c_peer, c_sem.at[j, 0, 0])

    own = table_ref[me]
    first = jnp.int32(0)
    bound = jnp.int32(0)
    for m in range(lengths_ref.shape[0]):
        bound = bound + lengths_ref[m]
        first = jnp.where(own >= bound, bound, first)
    slots = []
    for p in range(most):
        wanted = first + p
        slots.append(
            lax.fori_loop(
                0, seq_count,
                lambda s, a, wanted=wanted: jnp.where(table_ref[s] == wanted, s, a),
                jnp.int32(0),
            )
        )

    for start in range(0, most * block, block):
        gap = lax.broadcasted_iota(jnp.int32, (block, block), 1) - lax.broadcasted_iota(
            jnp.int32, (block, block), 0
        )
        bias[:, start:start + block] = jnp.where(gap <= (own - first) * block - start, 0.0, NEG_FILL)
    for k in range(len(offsets)):
        forward_z(0, k)
    x_own(1)
    x_own(2)
    forward_x(0, 0)
    forward_x(0, 1)
    for copy in q_copies:
        copy.wait()

    total_keys = prompt_total + most * block
    bounds = [(0, prompt_total)]
    at = prompt_total
    while at < total_keys:
        bounds.append((at, min(chunk, total_keys - at)))
        at += bounds[-1][1]
    pair = 2
    steps = group // pair

    part_width = pair * HEAD_SIZE

    def out_refs(j, i, owner):
        wide = part_width
        if isinstance(i, int) and i == steps:
            staged, result, start, wide = stage_p[j], pout_ref, 0, width
        else:
            staged, result, start = stage_a[j], aout_ref, i * part_width
        start = start if isinstance(start, int) else pl.multiple_of(start, part_width)
        cols = pl.ds(pl.multiple_of((owner * heads_kv + j) * width + start, wide), wide)
        return staged, result.at[:, cols], pl.ds(start, wide)

    def out_remote(j, i, k, owner):
        target = (head + k) % head_count
        staged, result, cols = out_refs(j, i, owner)
        return pltpu.make_async_remote_copy(
            src_ref=staged.at[target, :, cols], dst_ref=result,
            send_sem=out_send.at[j, i, k], recv_sem=out_recv.at[j, i, owner],
            device_id=(me, target), device_id_type=MESH,
        )

    def out_copy(j, i):
        staged, result, cols = out_refs(j, i, head)
        return pltpu.make_async_copy(staged.at[head, :, cols], result, out_local.at[j, i])

    def send_out(j, i):
        for k in range(1, head_count):
            out_remote(j, i, k, head).start()
        out_copy(j, i).start()

    for j in range(heads_kv):
        wait_c(j)
        for s in range(seq_count):
            rows = pl.ds(s * prompt_rows, prompt_rows)
            keys[rows, :] = pieces[j][s, 2 * block:2 * block + prompt_rows, :]
            values[rows, :] = pieces[j][s, 2 * block + prompt_rows:2 * (block + prompt_rows), :]
        for p in range(most):
            rows = pl.ds(prompt_total + p * block, block)
            keys[rows, :] = pieces[j][slots[p], 0:block, :]
            values[rows, :] = pieces[j][slots[p], block:2 * block, :]

        query = jnp.concatenate(
            [pqueries[:, (j * group + g) * HEAD_SIZE:(j * group + g + 1) * HEAD_SIZE] for g in range(group)],
            axis=0,
        )
        scores = score(query, keys[0:prompt_total, :])
        key_at = lax.broadcasted_iota(jnp.int32, scores.shape, 1)
        query_at = me * prompt_rows + lax.broadcasted_iota(jnp.int32, scores.shape, 0) % prompt_rows
        scores = jnp.where(key_at <= query_at, scores, NEG_FILL)
        state = softmax_step(None, scores, values[0:prompt_total, :])
        out = (state[2] / state[1]).astype(jnp.bfloat16)
        part = prompt_rows // head_count
        for g in range(group):
            for h in range(head_count):
                stage_p[j][h, :, g * HEAD_SIZE:(g + 1) * HEAD_SIZE] = out[
                    g * prompt_rows + h * part:g * prompt_rows + (h + 1) * part, :
                ]

        def first_pass(g, u):
            cols = pl.ds(pl.multiple_of((j * group + g) * HEAD_SIZE, HEAD_SIZE), HEAD_SIZE)
            query = queries[:, cols]
            peak = None
            for start, size in bounds:
                raw = lax.dot_general(
                    query, keys[start:start + size, :], (((1,), (1,)), ((), ())),
                    preferred_element_type=jnp.float32,
                )
                if start >= prompt_total:
                    raw = raw + bias[:, start - prompt_total:start - prompt_total + size]
                score_bufs[u][:, start:start + size] = raw
                for lane in range(0, size, HEAD_SIZE):
                    strip = raw[:, lane:lane + HEAD_SIZE]
                    peak = strip if peak is None else jnp.maximum(peak, strip)
            peaks[u][...] = peak

        def second_pass(g, u):
            peak = jnp.max(peaks[u][...], axis=-1, keepdims=True) * SCALE
            total = mixed = None
            for start, size in bounds:
                weights = jnp.exp2(score_bufs[u][:, start:start + size] * SCALE - peak)
                for lane in range(0, size, HEAD_SIZE):
                    strip = weights[:, lane:lane + HEAD_SIZE]
                    total = strip if total is None else total + strip
                part = jnp.dot(
                    weights.astype(jnp.bfloat16), values[start:start + size, :],
                    preferred_element_type=jnp.float32,
                )
                mixed = part if mixed is None else mixed + part
            out = (mixed / jnp.sum(total, axis=-1, keepdims=True)).astype(jnp.bfloat16)
            cols = pl.ds(pl.multiple_of(g * HEAD_SIZE, HEAD_SIZE), HEAD_SIZE)
            share = block // head_count
            for h in range(head_count):
                stage_a[j][h, :, cols] = out[h * share:(h + 1) * share, :]

        def hooks(i):
            @pl.when(i == 0)
            def _():
                send_out(j, steps)

            @pl.when(i > 0)
            def _():
                send_out(j, i - 1)

            third = -(-len(offsets) // 3)
            everything = list(range(len(offsets)))
            plan = [[] for _ in range(steps)]
            if j == 0:
                plan[0] += [(1, k) for k in everything] + [(3, None)]
                plan[1] += [(2, k) for k in everything[:third]]
                plan[2] += [(2, k) for k in everything[third:2 * third]]
            elif j == 1:
                plan[0] += [(2, k) for k in everything[2 * third:]]
            if j > 0:
                plan[1] += [(j + 2, k) for k in everything[:third]]
                plan[2] += [(j + 2, k) for k in everything[third:]] + [(j + 3, None)]
            for at, actions in enumerate(plan):
                @pl.when(i == at)
                def _(at=at, actions=actions):
                    for target, k in actions:
                        if k is None:
                            x_own(target)
                        else:
                            forward_z(target, k)
                    if at >= steps - 2:
                        forward_x(j + 1, at - (steps - 2))

        def step(i, carry):
            first_pass(2 * i + 1, 1)
            second_pass(2 * i, 0)
            first_pass(jnp.minimum(2 * i + 2, group - 1), 0)
            second_pass(2 * i + 1, 1)
            hooks(i)
            return carry

        first_pass(0, 0)
        lax.fori_loop(0, steps, step, 0)

        send_out(j, steps - 1)

    def out_parts():
        for j in range(heads_kv):
            for i in range(steps + 1):
                yield j, i

    for j, i in out_parts():
        out_copy(j, i).wait()
    for j, i in out_parts():
        for k in range(1, head_count):
            out_remote(j, i, k, (head + k) % head_count).wait_recv()
    for j in range(heads_kv):
        if relayed:
            for k in range(2):
                wait_sent(pieces[j].at[me], z_sem.at[j, k], c_peer, head)

            @pl.when(inner == 1)
            def _(j=j):
                for k in range(2):
                    wait_sent(pieces[j].at[me], z_sem.at[j, 2 + k], c_peer, head)
        else:
            for k in offsets:
                wait_sent(pieces[j].at[me], z_sem.at[j, k], c_peer, head)
        for k in range(z_count):
            wait_sent(pieces[j].at[me], x_sem.at[j, k], c_peer, head)
            for n in range(2):
                wait_sent(pieces[j].at[me], c_sem.at[j, n, k], c_peer, head)
    for j, i in out_parts():
        for k in range(1, head_count):
            out_remote(j, i, k, (head + k) % head_count).wait_send()


def wait_sent(ref, sem, peer, head):
    pltpu.make_async_remote_copy(
        src_ref=ref, dst_ref=ref, send_sem=sem, recv_sem=sem,
        device_id=(peer, head), device_id_type=MESH,
    ).wait_send()


def on_device(mesh_shape, pq, pk, pv, rq, rk, rv, lengths, table):
    seq_count, head_count = mesh_shape["seq"], mesh_shape["head"]
    heads_kv = rk.shape[1] // HEAD_SIZE
    group = rq.shape[1] // rk.shape[1]
    block, prompt_rows = rq.shape[0], pq.shape[0]
    most = table.shape[0] // 2
    width = group * HEAD_SIZE
    z_count = seq_count // 4
    total = prompt_rows * seq_count + most * block
    dma = pltpu.SemaphoreType.DMA
    any_space = pl.BlockSpec(memory_space=pl.ANY)
    smem = pl.BlockSpec(memory_space=pltpu.SMEM)
    return pl.pallas_call(
        functools.partial(kernel, seq_count, head_count, heads_kv, group, most, 512),
        out_shape=(
            jax.ShapeDtypeStruct((prompt_rows // head_count, rq.shape[1] * head_count), jnp.bfloat16),
            jax.ShapeDtypeStruct((block // head_count, rq.shape[1] * head_count), jnp.bfloat16),
        ),
        in_specs=[smem] * 2 + [any_space] * 6,
        out_specs=(any_space, any_space),
        scratch_shapes=(
            [pltpu.VMEM((seq_count, 2 * (block + prompt_rows), HEAD_SIZE), jnp.bfloat16)] * heads_kv
            + [pltpu.VMEM((head_count, block // head_count, width), jnp.bfloat16)] * heads_kv
            + [pltpu.VMEM((head_count, prompt_rows // head_count, width), jnp.bfloat16)] * heads_kv
            + [
                pltpu.VMEM((total, HEAD_SIZE), jnp.bfloat16),
                pltpu.VMEM((total, HEAD_SIZE), jnp.bfloat16),
                pltpu.VMEM(rq.shape, jnp.bfloat16),
                pltpu.VMEM(pq.shape, jnp.bfloat16),
                dma((heads_kv, 4)),
                dma((2,)),
                dma((heads_kv, seq_count)),
                dma((heads_kv, max(z_count, 4))),
                dma((heads_kv, z_count)),
                dma((heads_kv, 2, z_count)),
                dma((heads_kv, group // 2 + 1, head_count)),
                dma((heads_kv, group // 2 + 1, head_count)),
                dma((heads_kv, group // 2 + 1)),
                pltpu.VMEM((block, most * block), jnp.float32),
            ]
            + [pltpu.VMEM((block, total), jnp.float32)] * 2
            + [pltpu.VMEM((block, HEAD_SIZE), jnp.float32)] * 2
        ),
        compiler_params=pltpu.CompilerParams(
            collective_id=0, has_side_effects=True, vmem_limit_bytes=60 * 1024 * 1024
        ),
    )(lengths, table, pq, pk, pv, rq, rk, rv)


def solution(mesh):
    sharded = P("seq", "head")
    out = P(("seq", "head"), None)
    return jax.shard_map(
        functools.partial(on_device, dict(mesh.shape)), mesh=mesh,
        in_specs=(sharded,) * 6 + (P(), P()), out_specs=(out, out), check_vma=False,
    )
```
